32 devices in a mesh: segment: 4 (over x, core), dp: 8 (over z, y).
Axes of the slice: x: 2, y: 2, z: 4, core: 2. Of those that a mesh axis runs over, the one named last changes fastest.
Arguments:
- embeds: bfloat16 [2, 8, 128, 4096], P(None, 'dp'), may hold values from -6 to 6
- base_weight: bfloat16 [4, 4096, 4096], P('segment', 'dp'), may hold values from -0.09375 to 0.09375
- norm_gain: float32 [4, 4096], P('segment'), may hold values from 0.25 to 1.75
- skill_down: bfloat16 [4, 16, 8, 4096], P('segment'), may hold values from -0.09375 to 0.09375
- skill_up: bfloat16 [4, 16, 8, 4096], P('segment'), may hold values from -2 to 2
- task_ids: int32 [2, 8], replicated, may hold values from 0 to 1835
- allocation: int32 [1836, 16], replicated, may hold values 0 or 1
- target_lengths: int32 [2, 8], replicated, may hold values from 1 to 128
- cotangent: bfloat16 [2, 8, 128, 4096], P(None, 'dp'), may hold values from -6 to 6
Outputs:
- hidden: bfloat16 [4, 2, 8, 128, 4096], P('segment', None, 'dp')
- input_grads: bfloat16 [4, 2, 8, 128, 4096], P('segment', None, 'dp')
- grad_down: float32 [4, 16, 8, 4096], P('segment', None, None, 'dp')
- grad_up: float32 [4, 16, 8, 4096], P('segment', None, None, 'dp')
The draws below stay inside these ranges and needn't reach their ends.
All inputs are finite; a program needn't handle non-finite values.
Results may differ from the reference program's by a relative error of at most 0.019.
Values may be sent and summed in bfloat16 or wider, within the bound.
No kernel may reach another device: no remote copies, remote signals or barrier semaphores. Data moves between devices by JAX's collectives and lax.ppermute only.
A program may use at most 192 MiB of HBM per device.

```python
import jax
import jax.numpy as jnp
from jax import lax

D = 4096
SKILLS = 16
RANK = 8
TASKS = 1836
MICRO = 2
ROWS = 128
N_SEGMENT = 4
N_DP = 8


def with_ends(drawn, key, least, high):
    index_at = [jax.random.randint(jax.random.fold_in(key, axis), (), 0, length) for axis, length in enumerate(drawn.shape)]
    main_axis = drawn.shape.index(max(drawn.shape))
    next_to = index_at[:main_axis] + [(index_at[main_axis] + 1) % drawn.shape[main_axis]] + index_at[main_axis + 1:]
    return drawn.at[tuple(index_at)].set(least).at[tuple(next_to)].set(high)


def levels(stream_key, extent, pieces, least, top_value):
    factor_of = 1.0
    for position, parts in pieces:
        heights = jax.random.uniform(jax.random.fold_in(jax.random.fold_in(stream_key, 6), position), (parts,), jnp.float32, least / len(pieces), top_value / len(pieces))
        factor_of = factor_of * jnp.repeat(jnp.exp(heights), extent[position] // parts).reshape((-1,) + (1,) * (len(extent) - 1 - position))
    return factor_of


def gaussian(stream_key, dims, spread, reach, shards=(), held_as=jnp.bfloat16):
    factor_of = levels(stream_key, dims, shards, -0.22, 0.18) if shards else 1.0
    array = jax.random.normal(stream_key, dims, jnp.float32) * spread * factor_of
    return jnp.minimum(jnp.maximum(array, -reach), reach).astype(held_as)


def setup_inputs(seed: int = 0) -> dict:
    keys = jax.random.split(jax.random.key(seed), 10)
    embeds = gaussian(keys[0], (MICRO, N_DP, ROWS, D), 1.0, 6.0, ((1, 8),))
    base_weight = gaussian(keys[1], (N_SEGMENT, D, D), D ** -0.5, 0.09375, ((0, 4), (1, 8)))
    norm_gain = jnp.clip(1.0 + 0.15 * jax.random.normal(keys[2], (N_SEGMENT, D), jnp.float32), 0.25, 1.75)
    skill_down = gaussian(keys[3], (N_SEGMENT, SKILLS, RANK, D), D ** -0.5, 0.09375, ((0, 4),))
    skill_up = gaussian(keys[4], (N_SEGMENT, SKILLS, RANK, D), RANK ** -0.5, 2.0, ((0, 4),))
    task_ids = with_ends(jax.random.randint(keys[5], (MICRO, N_DP), 0, TASKS), jax.random.fold_in(keys[5], 1), 0, TASKS - 1).astype(jnp.int32)
    allocation = with_ends((jax.random.randint(keys[6], (TASKS, SKILLS), 0, 2) < 1).astype(jnp.int32), jax.random.fold_in(keys[6], 1), 0, 1)
    target_lengths = with_ends(jax.random.randint(keys[7], (MICRO, N_DP), 1, ROWS + 1), jax.random.fold_in(keys[7], 1), 1, ROWS).astype(jnp.int32)
    cotangent = gaussian(keys[8], (MICRO, N_DP, ROWS, D), 1.0, 6.0, ((1, 8),))
    return {"embeds": embeds, "base_weight": base_weight, "norm_gain": norm_gain, "skill_down": skill_down, "skill_up": skill_up, "task_ids": task_ids, "allocation": allocation, "target_lengths": target_lengths, "cotangent": cotangent}


EPS = 1e-06

def mixing_table(task_ids, allocation):
    onehot = (task_ids[..., None] == jnp.arange(TASKS, dtype=jnp.int32)).astype(jnp.float32)
    alloc = allocation.astype(jnp.float32)
    counts = jnp.maximum(lax.optimization_barrier(jnp.sum(alloc, axis=1, keepdims=True)), 1.0)
    return jnp.einsum('...t,ts->...s', onehot, alloc / counts, precision=lax.Precision.HIGHEST)

def prepare(x, gain, down_t):
    xf = x.astype(jnp.float32)
    inv = lax.rsqrt(lax.optimization_barrier(jnp.mean(xf * xf, axis=-1, keepdims=True)) + EPS)
    normed = (xf * inv * gain).astype(jnp.bfloat16)
    low = jnp.dot(normed, down_t.T, preferred_element_type=jnp.float32).astype(jnp.bfloat16)
    return (normed, low, inv)

def forward_one(x, weight, gain, down_t, up_t):
    normed, low, inv = prepare(x, gain, down_t)
    total = x.astype(jnp.float32) + jnp.dot(normed, weight, preferred_element_type=jnp.float32)
    total = total + jnp.dot(low, up_t, preferred_element_type=jnp.float32)
    return total.astype(jnp.bfloat16)

def backward_core(x, normed, low, inv, grad_out, weight, gain, down_t, up_t):
    g_low = jnp.dot(grad_out, up_t.T, preferred_element_type=jnp.float32).astype(jnp.bfloat16)
    dnorm = jnp.dot(grad_out, weight.T, preferred_element_type=jnp.float32)
    dnorm = dnorm + jnp.dot(g_low, down_t, preferred_element_type=jnp.float32)
    seq_down = jnp.dot(g_low.T, normed, preferred_element_type=jnp.float32)
    seq_up = jnp.dot(low.T, grad_out, preferred_element_type=jnp.float32)
    xf = x.astype(jnp.float32)
    scaled = gain * dnorm
    grad_in = grad_out.astype(jnp.float32) + inv * scaled - xf * inv * inv * inv * lax.optimization_barrier(jnp.mean(xf * scaled, axis=-1, keepdims=True))
    return (grad_in.astype(jnp.bfloat16), seq_down, seq_up)

def backward_one(x, grad_out, weight, gain, down_t, up_t):
    normed, low, inv = prepare(x, gain, down_t)
    return backward_core(x, normed, low, inv, grad_out, weight, gain, down_t, up_t)

def reference(embeds, base_weight, norm_gain, skill_down, skill_up, task_ids, allocation, target_lengths, cotangent):
    mix = mixing_table(task_ids, allocation)
    flat_mix = mix.reshape(MICRO * N_DP, SKILLS)
    state = embeds.reshape(MICRO * N_DP, ROWS, D)
    downs, ups, inputs, outputs = ([], [], [], [])
    for level in range(N_SEGMENT):
        down_t = jnp.einsum('qs,srd->qrd', flat_mix, skill_down[level].astype(jnp.float32), precision=lax.Precision.HIGHEST).astype(jnp.bfloat16)
        up_t = jnp.einsum('qs,srd->qrd', flat_mix, skill_up[level].astype(jnp.float32), precision=lax.Precision.HIGHEST).astype(jnp.bfloat16)
        downs.append(down_t)
        ups.append(up_t)
        inputs.append(state)
        state = jax.vmap(forward_one, in_axes=(0, None, None, 0, 0))(state, base_weight[level], norm_gain[level], down_t, up_t)
        outputs.append(state)
    mask = jnp.arange(ROWS, dtype=jnp.int32)[None, None, :] < target_lengths[..., None]
    grad_state = (cotangent * mask[..., None].astype(jnp.bfloat16)).reshape(MICRO * N_DP, ROWS, D)
    grads_in = [None] * N_SEGMENT
    grads_down = [None] * N_SEGMENT
    grads_up = [None] * N_SEGMENT
    for level in reversed(range(N_SEGMENT)):
        grad_state, seq_down, seq_up = jax.vmap(backward_one, in_axes=(0, 0, None, None, 0, 0))(inputs[level], grad_state, base_weight[level], norm_gain[level], downs[level], ups[level])
        grads_in[level] = grad_state
        part_down = jnp.einsum('mjs,mjrd->jsrd', mix, seq_down.reshape(MICRO, N_DP, RANK, D), precision=lax.Precision.HIGHEST)
        part_up = jnp.einsum('mjs,mjrd->jsrd', mix, seq_up.reshape(MICRO, N_DP, RANK, D), precision=lax.Precision.HIGHEST)
        grads_down[level] = lax.optimization_barrier(jnp.sum(part_down.astype(jnp.bfloat16).astype(jnp.float32), axis=0))
        grads_up[level] = lax.optimization_barrier(jnp.sum(part_up.astype(jnp.bfloat16).astype(jnp.float32), axis=0))
    hidden = jnp.stack(outputs).reshape(N_SEGMENT, MICRO, N_DP, ROWS, D)
    input_grads = jnp.stack(grads_in).reshape(N_SEGMENT, MICRO, N_DP, ROWS, D)
    return (hidden, input_grads, jnp.stack(grads_down), jnp.stack(grads_up))
```

```python
import jax
import jax.numpy as jnp
from jax import lax
from jax.sharding import PartitionSpec as P

EPS = 1e-06


def snake(count):
    inner = max(d for d in range(1, count + 1) if count % d == 0 and d * d <= count)
    outer = count // inner
    if inner == 1 or outer == 1:
        return list(range(count))
    if inner % 2:
        return [z * inner + (y if z % 2 == 0 else inner - 1 - y) for z in range(outer) for y in range(inner)]
    back = []
    for y in range(inner):
        column = [z * inner + y for z in range(1, outer)]
        back += column if y % 2 == 0 else column[::-1]
    return [y for y in range(1)] + back + [y for y in range(inner - 1, 0, -1)]


def prepare(x, gain, down):
    xf = x.astype(jnp.float32)
    inv = lax.rsqrt(jnp.mean(xf * xf, axis=-1, keepdims=True) + EPS)
    normed = (xf * inv * gain).astype(jnp.bfloat16)
    low = jnp.einsum("mtd,mrd->mtr", normed, down, preferred_element_type=jnp.float32).astype(jnp.bfloat16)
    return (normed, low, inv)


def wide(rows, weight):
    flat = rows.reshape(-1, rows.shape[-1])
    return jnp.dot(flat, weight, preferred_element_type=jnp.float32).reshape(rows.shape[:-1] + (weight.shape[1],))


def forward(x, weight, gain, down, up):
    normed, low, inv = prepare(x, gain, down)
    total = x.astype(jnp.float32) + wide(normed, weight)
    total = total + jnp.einsum("mtr,mrd->mtd", low, up, preferred_element_type=jnp.float32)
    return total.astype(jnp.bfloat16)


def backward(x, inv, grad, weight, gain, down, up):
    g_low = jnp.einsum("mtd,mrd->mtr", grad, up, preferred_element_type=jnp.float32).astype(jnp.bfloat16)
    dnorm = wide(grad, weight.T)
    dnorm = dnorm + jnp.einsum("mtr,mrd->mtd", g_low, down, preferred_element_type=jnp.float32)
    xf = x.astype(jnp.float32)
    scaled = gain * dnorm
    grad_in = (
        grad.astype(jnp.float32)
        + inv * scaled
        - xf * inv * inv * inv * jnp.mean(xf * scaled, axis=-1, keepdims=True)
    )
    return grad_in.astype(jnp.bfloat16)


def sequence_grads(normed, low, grad, up):
    g_low = jnp.einsum("mtd,mrd->mtr", grad, up, preferred_element_type=jnp.float32).astype(jnp.bfloat16)
    seq_down = jnp.einsum("mtr,mtd->mrd", g_low, normed, preferred_element_type=jnp.float32)
    seq_up = jnp.einsum("mtr,mtd->mrd", low, grad, preferred_element_type=jnp.float32)
    return seq_down, seq_up


def shards(
    embeds,
    base_weight,
    norm_gain,
    skill_down,
    skill_up,
    task_ids,
    allocation,
    target_lengths,
    cotangent,
):
    segments = lax.axis_size("segment")
    members = lax.axis_size("dp")
    segment = lax.axis_index("segment")
    member = lax.axis_index("dp")
    order = snake(members)
    gathered = lax.all_gather(base_weight[0], "dp", axis=0, axis_index_groups=[order])
    place_of = [order.index(j) for j in range(members)]
    weight = jnp.concatenate([gathered[p] for p in place_of], axis=0)
    gain = norm_gain[0]
    rows = embeds.shape[2]
    width = embeds.shape[3]
    onehot = (task_ids[..., None] == jnp.arange(allocation.shape[0], dtype=jnp.int32)).astype(jnp.float32)
    alloc = allocation.astype(jnp.float32)
    counts = jnp.maximum(jnp.sum(alloc, axis=1, keepdims=True), 1.0)
    mix_all = jnp.einsum("mjt,ts->mjs", onehot, alloc / counts, precision=lax.Precision.HIGHEST)
    mix = lax.dynamic_index_in_dim(mix_all, member, 1, keepdims=False)
    lengths = lax.dynamic_index_in_dim(target_lengths, member, 1, keepdims=False)
    down = jnp.einsum(
        "ms,srd->mrd", mix, skill_down[0].astype(jnp.float32), precision=lax.Precision.HIGHEST
    ).astype(jnp.bfloat16)
    up = jnp.einsum(
        "ms,srd->mrd", mix, skill_up[0].astype(jnp.float32), precision=lax.Precision.HIGHEST
    ).astype(jnp.bfloat16)
    live = jnp.arange(rows, dtype=jnp.int32)[None, :] < lengths[:, None]
    x = embeds[:, 0]
    for k in range(segments - 1):
        result = forward(x, weight, gain, down, up)
        moved = lax.ppermute(result, "segment", [(k, k + 1)])
        x = jnp.where(segment == k + 1, moved, x)
    hidden = forward(x, weight, gain, down, up)
    normed, low, inv = prepare(x, gain, down)
    grad = cotangent[:, 0] * live[..., None].astype(jnp.bfloat16)
    for k in range(segments - 1, 0, -1):
        result = backward(x, inv, grad, weight, gain, down, up)
        moved = lax.ppermute(result, "segment", [(k, k - 1)])
        grad = jnp.where(segment == k - 1, moved, grad)
    both = jnp.stack(sequence_grads(normed, low, grad, up)).astype(jnp.bfloat16)
    split = both.reshape(both.shape[:-1] + (members, width // members))
    parts = lax.all_to_all(split, "dp", split_axis=split.ndim - 2, concat_axis=0)
    grad_in = backward(x, inv, grad, weight, gain, down, up)
    mixed = jnp.einsum("mjs,jfmrd->fjsrd", mix_all, parts.astype(jnp.float32), precision=lax.Precision.HIGHEST)
    total = jnp.sum(mixed.astype(jnp.bfloat16).astype(jnp.float32), axis=1)
    return (hidden[None, :, None], grad_in[None, :, None], total[0][None], total[1][None])


def solution(mesh):
    in_specs = (
        P(None, "dp", None, None),
        P("segment", "dp", None),
        P("segment", None),
        P("segment", None, None, None),
        P("segment", None, None, None),
        P(),
        P(),
        P(),
        P(None, "dp", None, None),
    )
    out_specs = (
        P("segment", None, "dp", None, None),
        P("segment", None, "dp", None, None),
        P("segment", None, None, "dp"),
        P("segment", None, None, "dp"),
    )
    return jax.shard_map(shards, mesh=mesh, in_specs=in_specs, out_specs=out_specs, check_vma=False)
```

```python
import functools

import jax
import jax.numpy as jnp
from jax import lax
from jax.experimental import pallas as pl
from jax.experimental.pallas import tpu as pltpu
from jax.sharding import PartitionSpec as P

EPS = 1e-06


def snake(count):
    inner = max(d for d in range(1, count + 1) if count % d == 0 and d * d <= count)
    outer = count // inner
    if inner == 1 or outer == 1:
        return list(range(count))
    if inner % 2:
        return [z * inner + (y if z % 2 == 0 else inner - 1 - y) for z in range(outer) for y in range(inner)]
    back = []
    for y in range(inner):
        column = [z * inner + y for z in range(1, outer)]
        back += column if y % 2 == 0 else column[::-1]
    return [y for y in range(1)] + back + [y for y in range(inner - 1, 0, -1)]


def fold(x):
    return x.astype(jnp.float32)


def row_scale(xf):
    return lax.rsqrt(jnp.mean(xf * xf, axis=-1, keepdims=True) + EPS)


def nt_dot(a, b):
    return lax.dot_general(a, b, (((1,), (1,)), ((), ())), preferred_element_type=jnp.float32)


def tn_dot(a, b):
    return lax.dot_general(a, b, (((0,), (0,)), ((), ())), preferred_element_type=jnp.float32)


def nn_dot(a, b):
    return jnp.dot(a, b, preferred_element_type=jnp.float32)


def here(k):
    return lax.axis_index("segment") == k


def own(low, micro):
    count, columns = low.shape
    row = lax.broadcasted_iota(jnp.int32, low.shape, 0) // (count // micro)
    column = lax.broadcasted_iota(jnp.int32, low.shape, 1) // (columns // micro)
    return jnp.where(row == column, low, 0.0).astype(jnp.bfloat16)


def pick(k, moved, kept, chosen):
    @pl.when(here(k))
    def _():
        chosen[...] = moved[...]

    @pl.when(jnp.logical_not(here(k)))
    def _():
        chosen[...] = kept[...]


def forward_body(order, micro, k, moved, kept, gain, down, up, weight, out, chosen, normed, low):
    step = pl.program_id(0)
    tile = out.shape[-1]
    rows = kept.shape[0] // micro
    part = weight.shape[1]

    @pl.when(step == 0)
    def _():
        pick(k, moved, kept, chosen)
        total = jnp.zeros(low.shape, jnp.float32)
        inv = row_scale(fold(chosen[...]))
        for slot, source in enumerate(order):
            span = slice(source * part, (source + 1) * part)
            h = (fold(chosen[:, span]) * inv * gain[:, span]).astype(jnp.bfloat16)
            normed[:, slot * part : (slot + 1) * part] = h
            total = total + nt_dot(h, down[:, span])
        low[...] = own(total, micro)

    columns = pl.ds(pl.multiple_of(step * tile, tile), tile)
    total = nn_dot(normed[...], weight[...].reshape(-1, tile)) + nn_dot(low[...], up[...])
    out[...] = (fold(chosen[:, columns]) + total).astype(jnp.bfloat16)


def forward_step(order, micro, tile, k, moved, kept, gain, down, up, weight):
    ranks, width = down.shape
    count = kept.shape[0]
    whole = pl.BlockSpec((count, width), lambda n: (0, 0), pipeline_mode=pl.Buffered(1))
    return pl.pallas_call(
        functools.partial(forward_body, order, micro, k),
        grid=(width // tile,),
        in_specs=[
            whole,
            whole,
            pl.BlockSpec((1, width), lambda n: (0, 0)),
            pl.BlockSpec((ranks, width), lambda n: (0, 0)),
            pl.BlockSpec((ranks, tile), lambda n: (0, n)),
            pl.BlockSpec(weight.shape[:2] + (tile,), lambda n: (0, 0, n)),
        ],
        out_specs=[
            pl.BlockSpec((count, tile), lambda n: (0, n)),
            pl.BlockSpec((count, width), lambda n: (0, 0)),
        ],
        out_shape=[jax.ShapeDtypeStruct((count, width), jnp.bfloat16)] * 2,
        scratch_shapes=[pltpu.VMEM((count, width), jnp.bfloat16), pltpu.VMEM((count, ranks), jnp.bfloat16)],
        compiler_params=pltpu.CompilerParams(dimension_semantics=("arbitrary",), vmem_limit_bytes=60000 * 1024),
        cost_estimate=pl.CostEstimate(
            flops=2 * count * width * width, transcendentals=0, bytes_accessed=2 * width * width
        ),
        name="forward_step",
    )(moved, kept, gain, down, up, weight)


def backward_body(order, micro, k, moved, kept, x, gain, down, up, weight, out, chosen, summed, low, inv, dots):
    step = pl.program_id(0)
    part = weight.shape[1]

    @pl.when(step == 0)
    def _():
        pick(k, moved, kept, chosen)
        inv[...] = row_scale(fold(x[...]))
        low[...] = own(nt_dot(chosen[...], up[...]), micro)
        dots[...] = jnp.zeros_like(dots)

    source = jnp.int32(order[0])
    for slot in range(1, len(order)):
        source = jnp.where(step == slot, jnp.int32(order[slot]), source)
    columns = pl.ds(pl.multiple_of(source * part, part), part)
    total = nt_dot(chosen[...], weight[0]) + nn_dot(low[...], down[:, columns])
    scaled = total * gain[:, columns]
    dots[...] += jnp.sum(fold(x[:, columns]) * scaled, axis=-1, keepdims=True)
    summed[:, columns] = fold(chosen[:, columns]) + inv[...] * scaled

    @pl.when(step == pl.num_programs(0) - 1)
    def _():
        scale = inv[...]
        shift = scale * scale * scale * dots[...] * (1.0 / x.shape[1])
        out[...] = (summed[...] - fold(x[...]) * shift).astype(jnp.bfloat16)


def backward_step(order, micro, k, moved, kept, x, gain, down, up, weight):
    ranks, width = down.shape
    count = kept.shape[0]
    whole = pl.BlockSpec((count, width), lambda n: (0, 0), pipeline_mode=pl.Buffered(1))
    return pl.pallas_call(
        functools.partial(backward_body, order, micro, k),
        grid=(weight.shape[0],),
        in_specs=[
            whole,
            whole,
            whole,
            pl.BlockSpec((1, width), lambda n: (0, 0)),
            pl.BlockSpec((ranks, width), lambda n: (0, 0)),
            pl.BlockSpec((ranks, width), lambda n: (0, 0)),
            pl.BlockSpec((1,) + weight.shape[1:], lambda n: (n, 0, 0)),
        ],
        out_specs=[whole_out(count, width), whole_out(count, width)],
        out_shape=[jax.ShapeDtypeStruct((count, width), jnp.bfloat16)] * 2,
        scratch_shapes=[
            pltpu.VMEM((count, width), jnp.float32),
            pltpu.VMEM((count, ranks), jnp.bfloat16),
            pltpu.VMEM((count, 1), jnp.float32),
            pltpu.VMEM((count, 1), jnp.float32),
        ],
        compiler_params=pltpu.CompilerParams(dimension_semantics=("arbitrary",), vmem_limit_bytes=60000 * 1024),
        cost_estimate=pl.CostEstimate(
            flops=2 * count * width * width, transcendentals=0, bytes_accessed=2 * width * width
        ),
        name="backward_step",
    )(moved, kept, x, gain, down, up, weight)


def whole_out(count, width):
    return pl.BlockSpec((count, width), lambda n: (0, 0))


def sequence_body(micro, k, moved, kept, x, gain, down, up, out):
    members = out.shape[0]
    rank = down.shape[0] // micro
    rows = x.shape[0] // micro
    part = x.shape[1] // members
    for m in range(micro):
        block = slice(m * rows, (m + 1) * rows)
        ranks = slice(m * rank, (m + 1) * rank)
        g = jnp.where(here(k), moved[block, :], kept[block, :])
        xf = fold(x[block, :])
        h = (xf * row_scale(xf) * gain[...]).astype(jnp.bfloat16)
        low = nt_dot(h, down[ranks, :]).astype(jnp.bfloat16)
        g_low = nt_dot(g, up[ranks, :]).astype(jnp.bfloat16)
        for f, value in enumerate((tn_dot(g_low, h), tn_dot(low, g))):
            start = (f * micro + m) * rank
            for j in range(members):
                out[j, start : start + rank, :] = value[:, j * part : (j + 1) * part].astype(jnp.bfloat16)


def sequence_step(members, micro, k, moved, kept, x, gain, down, up):
    ranks, width = down.shape
    vmem = pl.BlockSpec(memory_space=pltpu.VMEM)
    return pl.pallas_call(
        functools.partial(sequence_body, micro, k),
        in_specs=[vmem] * 6,
        out_specs=vmem,
        out_shape=jax.ShapeDtypeStruct((members, 2 * ranks, width // members), jnp.bfloat16),
        compiler_params=pltpu.CompilerParams(vmem_limit_bytes=60000 * 1024),
        name="sequence_step",
    )(moved, kept, x, gain, down, up)


def shards(
    embeds,
    base_weight,
    norm_gain,
    skill_down,
    skill_up,
    task_ids,
    allocation,
    target_lengths,
    cotangent,
):
    segments = lax.axis_size("segment")
    members = lax.axis_size("dp")
    segment = lax.axis_index("segment")
    member = lax.axis_index("dp")
    order = snake(members)
    weight = lax.all_gather(base_weight[0], "dp", axis=0, axis_index_groups=[order])
    gain = norm_gain
    rows = embeds.shape[2]
    width = embeds.shape[3]
    onehot = (task_ids[..., None] == jnp.arange(allocation.shape[0], dtype=jnp.int32)).astype(jnp.float32)
    alloc = allocation.astype(jnp.float32)
    counts = jnp.maximum(jnp.sum(alloc, axis=1, keepdims=True), 1.0)
    mix_all = jnp.einsum("mjt,ts->mjs", onehot, alloc / counts, precision=lax.Precision.HIGHEST)
    mix = lax.dynamic_index_in_dim(mix_all, member, 1, keepdims=False)
    lengths = lax.dynamic_index_in_dim(target_lengths, member, 1, keepdims=False)
    down = jnp.einsum(
        "ms,srd->mrd", mix, skill_down[0].astype(jnp.float32), precision=lax.Precision.HIGHEST
    ).astype(jnp.bfloat16)
    up = jnp.einsum(
        "ms,srd->mrd", mix, skill_up[0].astype(jnp.float32), precision=lax.Precision.HIGHEST
    ).astype(jnp.bfloat16)
    live = jnp.arange(rows, dtype=jnp.int32)[None, :] < lengths[:, None]
    micro = embeds.shape[0]
    x = embeds.reshape(micro * rows, width)
    grad = (cotangent[:, 0] * live[..., None].astype(jnp.bfloat16)).reshape(micro * rows, width)
    tile = min(width, max(128, (1 << 22) // (2 * width)))
    down = down.reshape(-1, width)
    up = up.reshape(-1, width)
    weight, grad, down, up = lax.optimization_barrier((weight, grad, down, up))
    last = segments - 1

    hidden = moved = x
    for k in range(last):
        hidden, x = forward_step(order, micro, tile, k, moved, x, gain, down, up, weight)
        moved = lax.ppermute(hidden, "segment", [(k, k + 1)])
    x = jnp.where(segment == last, moved, x)
    moved = grad
    for k in range(last, 0, -1):
        result, grad = backward_step(order, micro, k, moved, grad, x, gain, down, up, weight)
        moved = lax.ppermute(result, "segment", [(k, k - 1)])
        if k == last:
            hidden = lax.cond(
                segment == last,
                lambda: forward_step(order, micro, tile, last, x, x, gain, down, up, weight)[0],
                lambda: hidden,
            )
    both = sequence_step(members, micro, 0, moved, grad, x, gain, down, up)
    parts = lax.all_to_all(both, "dp", split_axis=0, concat_axis=0, tiled=True)
    grad_in, _ = backward_step(order, micro, 0, moved, grad, x, gain, down, up, weight)
    hidden = hidden.reshape(micro, rows, width)
    grad_in = grad_in.reshape(micro, rows, width)
    parts = parts.reshape(members, 2, micro, -1, width // members)
    mixed = jnp.einsum("mjs,jfmrd->fjsrd", mix_all, parts.astype(jnp.float32), precision=lax.Precision.HIGHEST)
    total = jnp.sum(mixed.astype(jnp.bfloat16).astype(jnp.float32), axis=1)
    return (hidden[None, :, None], grad_in[None, :, None], total[0][None], total[1][None])


def solution(mesh):
    in_specs = (
        P(None, "dp", None, None),
        P("segment", "dp", None),
        P("segment", None),
        P("segment", None, None, None),
        P("segment", None, None, None),
        P(),
        P(),
        P(),
        P(None, "dp", None, None),
    )
    out_specs = (
        P("segment", None, "dp", None, None),
        P("segment", None, "dp", None, None),
        P("segment", None, None, "dp"),
        P("segment", None, None, "dp"),
    )
    return jax.shard_map(shards, mesh=mesh, in_specs=in_specs, out_specs=out_specs, check_vma=False)
```

```python
import functools

import jax
import jax.numpy as jnp
from jax import lax
from jax.experimental import pallas as pl
from jax.experimental.pallas import tpu as pltpu
from jax.sharding import PartitionSpec as P

EPS = 1e-06


def snake(count):
    inner = max(d for d in range(1, count + 1) if count % d == 0 and d * d <= count)
    outer = count // inner
    if inner == 1 or outer == 1:
        return list(range(count))
    if inner % 2:
        return [z * inner + (y if z % 2 == 0 else inner - 1 - y) for z in range(outer) for y in range(inner)]
    back = []
    for y in range(inner):
        column = [z * inner + y for z in range(1, outer)]
        back += column if y % 2 == 0 else column[::-1]
    return [y for y in range(1)] + back + [y for y in range(inner - 1, 0, -1)]


def fold(x):
    return x.astype(jnp.float32)


def row_scale(xf):
    return lax.rsqrt(jnp.mean(xf * xf, axis=-1, keepdims=True) + EPS)


def nt_dot(a, b):
    return lax.dot_general(a, b, (((1,), (1,)), ((), ())), preferred_element_type=jnp.float32)


def tn_dot(a, b):
    return lax.dot_general(a, b, (((0,), (0,)), ((), ())), preferred_element_type=jnp.float32)


def nn_dot(a, b):
    return jnp.dot(a, b, preferred_element_type=jnp.float32)


def here(k):
    return lax.axis_index("segment") == k


def own(low, micro):
    count, columns = low.shape
    row = lax.broadcasted_iota(jnp.int32, low.shape, 0) // (count // micro)
    column = lax.broadcasted_iota(jnp.int32, low.shape, 1) // (columns // micro)
    return jnp.where(row == column, low, 0.0).astype(jnp.bfloat16)


def pick(k, moved, kept, chosen):
    @pl.when(here(k))
    def _():
        chosen[...] = moved[...]

    @pl.when(jnp.logical_not(here(k)))
    def _():
        chosen[...] = kept[...]


def forward_body(order, micro, k, moved, kept, gain, down, up, weight, out, chosen, normed, low):
    step = pl.program_id(0)
    tile = out.shape[-1]
    rows = kept.shape[0] // micro
    part = weight.shape[1]

    @pl.when(step == 0)
    def _():
        pick(k, moved, kept, chosen)
        total = jnp.zeros(low.shape, jnp.float32)
        inv = row_scale(fold(chosen[...]))
        for slot, source in enumerate(order):
            span = slice(source * part, (source + 1) * part)
            h = (fold(chosen[:, span]) * inv * gain[:, span]).astype(jnp.bfloat16)
            normed[:, slot * part : (slot + 1) * part] = h
            total = total + nt_dot(h, down[:, span])
        low[...] = own(total, micro)

    columns = pl.ds(pl.multiple_of(step * tile, tile), tile)
    total = nn_dot(normed[...], weight[...].reshape(-1, tile)) + nn_dot(low[...], up[...])
    out[...] = (fold(chosen[:, columns]) + total).astype(jnp.bfloat16)


def forward_step(order, micro, tile, k, moved, kept, gain, down, up, weight):
    ranks, width = down.shape
    count = kept.shape[0]
    whole = pl.BlockSpec((count, width), lambda n: (0, 0), pipeline_mode=pl.Buffered(1))
    return pl.pallas_call(
        functools.partial(forward_body, order, micro, k),
        grid=(width // tile,),
        in_specs=[
            whole,
            whole,
            pl.BlockSpec((1, width), lambda n: (0, 0)),
            pl.BlockSpec((ranks, width), lambda n: (0, 0)),
            pl.BlockSpec((ranks, tile), lambda n: (0, n)),
            pl.BlockSpec(weight.shape[:2] + (tile,), lambda n: (0, 0, n)),
        ],
        out_specs=[
            pl.BlockSpec((count, tile), lambda n: (0, n)),
            pl.BlockSpec((count, width), lambda n: (0, 0)),
        ],
        out_shape=[jax.ShapeDtypeStruct((count, width), jnp.bfloat16)] * 2,
        scratch_shapes=[pltpu.VMEM((count, width), jnp.bfloat16), pltpu.VMEM((count, ranks), jnp.bfloat16)],
        compiler_params=pltpu.CompilerParams(dimension_semantics=("arbitrary",), vmem_limit_bytes=60000 * 1024),
        cost_estimate=pl.CostEstimate(
            flops=2 * count * width * width, transcendentals=0, bytes_accessed=2 * width * width
        ),
        name="forward_step",
    )(moved, kept, gain, down, up, weight)


def backward_body(order, micro, k, moved, kept, x, gain, down, up, weight, out, chosen, summed, low, inv, dots):
    step = pl.program_id(0)
    part = weight.shape[1]

    @pl.when(step == 0)
    def _():
        pick(k, moved, kept, chosen)
        inv[...] = row_scale(fold(x[...]))
        low[...] = own(nt_dot(chosen[...], up[...]), micro)
        dots[...] = jnp.zeros_like(dots)

    together = weight.shape[0]
    for u in range(together):
        source = jnp.int32(order[u])
        for slot in range(together + u, len(order), together):
            source = jnp.where(step == slot // together, jnp.int32(order[slot]), source)
        columns = pl.ds(pl.multiple_of(source * part, part), part)
        total = nt_dot(chosen[...], weight[u]) + nn_dot(low[...], down[:, columns])
        scaled = total * gain[:, columns]
        dots[...] += jnp.sum(fold(x[:, columns]) * scaled, axis=-1, keepdims=True)
        summed[:, columns] = fold(chosen[:, columns]) + inv[...] * scaled

    @pl.when(step == pl.num_programs(0) - 1)
    def _():
        scale = inv[...]
        shift = scale * scale * scale * dots[...] * (1.0 / x.shape[1])
        out[...] = (summed[...] - fold(x[...]) * shift).astype(jnp.bfloat16)


def backward_step(order, micro, k, moved, kept, x, gain, down, up, weight):
    ranks, width = down.shape
    together = 2 if len(order) % 2 == 0 else 1
    count = kept.shape[0]
    whole = pl.BlockSpec((count, width), lambda n: (0, 0), pipeline_mode=pl.Buffered(1))
    return pl.pallas_call(
        functools.partial(backward_body, order, micro, k),
        grid=(weight.shape[0] // together,),
        in_specs=[
            whole,
            whole,
            whole,
            pl.BlockSpec((1, width), lambda n: (0, 0)),
            pl.BlockSpec((ranks, width), lambda n: (0, 0)),
            pl.BlockSpec((ranks, width), lambda n: (0, 0)),
            pl.BlockSpec((together,) + weight.shape[1:], lambda n: (n, 0, 0)),
        ],
        out_specs=[whole_out(count, width), whole_out(count, width)],
        out_shape=[jax.ShapeDtypeStruct((count, width), jnp.bfloat16)] * 2,
        scratch_shapes=[
            pltpu.VMEM((count, width), jnp.float32),
            pltpu.VMEM((count, ranks), jnp.bfloat16),
            pltpu.VMEM((count, 1), jnp.float32),
            pltpu.VMEM((count, 1), jnp.float32),
        ],
        compiler_params=pltpu.CompilerParams(dimension_semantics=("arbitrary",), vmem_limit_bytes=60000 * 1024),
        cost_estimate=pl.CostEstimate(
            flops=2 * count * width * width, transcendentals=0, bytes_accessed=2 * width * width
        ),
        name="backward_step",
    )(moved, kept, x, gain, down, up, weight)


def whole_out(count, width):
    return pl.BlockSpec((count, width), lambda n: (0, 0))


def sequence_body(micro, k, moved, kept, x, gain, down, up, out):
    members = out.shape[0]
    rank = down.shape[0] // micro
    rows = x.shape[0] // micro
    part = x.shape[1] // members
    for m in range(micro):
        block = slice(m * rows, (m + 1) * rows)
        ranks = slice(m * rank, (m + 1) * rank)
        g = jnp.where(here(k), moved[block, :], kept[block, :])
        xf = fold(x[block, :])
        h = (xf * row_scale(xf) * gain[...]).astype(jnp.bfloat16)
        low = nt_dot(h, down[ranks, :]).astype(jnp.bfloat16)
        g_low = nt_dot(g, up[ranks, :]).astype(jnp.bfloat16)
        for f, value in enumerate((tn_dot(g_low, h), tn_dot(low, g))):
            start = (f * micro + m) * rank
            for j in range(members):
                out[j, start : start + rank, :] = value[:, j * part : (j + 1) * part].astype(jnp.bfloat16)


def sequence_step(members, micro, k, moved, kept, x, gain, down, up):
    ranks, width = down.shape
    vmem = pl.BlockSpec(memory_space=pltpu.VMEM)
    return pl.pallas_call(
        functools.partial(sequence_body, micro, k),
        in_specs=[vmem] * 6,
        out_specs=vmem,
        out_shape=jax.ShapeDtypeStruct((members, 2 * ranks, width // members), jnp.bfloat16),
        compiler_params=pltpu.CompilerParams(vmem_limit_bytes=60000 * 1024),
        name="sequence_step",
    )(moved, kept, x, gain, down, up)


def shards(
    embeds,
    base_weight,
    norm_gain,
    skill_down,
    skill_up,
    task_ids,
    allocation,
    target_lengths,
    cotangent,
):
    segments = lax.axis_size("segment")
    members = lax.axis_size("dp")
    segment = lax.axis_index("segment")
    member = lax.axis_index("dp")
    order = snake(members)
    weight = lax.all_gather(base_weight[0], "dp", axis=0, axis_index_groups=[order])
    gain = norm_gain
    rows = embeds.shape[2]
    width = embeds.shape[3]
    onehot = (task_ids[..., None] == jnp.arange(allocation.shape[0], dtype=jnp.int32)).astype(jnp.float32)
    alloc = allocation.astype(jnp.float32)
    counts = jnp.maximum(jnp.sum(alloc, axis=1, keepdims=True), 1.0)
    mix_all = jnp.einsum("mjt,ts->mjs", onehot, alloc / counts, precision=lax.Precision.HIGHEST)
    mix = lax.dynamic_index_in_dim(mix_all, member, 1, keepdims=False)
    lengths = lax.dynamic_index_in_dim(target_lengths, member, 1, keepdims=False)
    down = jnp.einsum(
        "ms,srd->mrd", mix, skill_down[0].astype(jnp.float32), precision=lax.Precision.HIGHEST
    ).astype(jnp.bfloat16)
    up = jnp.einsum(
        "ms,srd->mrd", mix, skill_up[0].astype(jnp.float32), precision=lax.Precision.HIGHEST
    ).astype(jnp.bfloat16)
    live = jnp.arange(rows, dtype=jnp.int32)[None, :] < lengths[:, None]
    micro = embeds.shape[0]
    x = embeds.reshape(micro * rows, width)
    grad = (cotangent[:, 0] * live[..., None].astype(jnp.bfloat16)).reshape(micro * rows, width)
    tile = min(width, max(128, (1 << 23) // (2 * width)))
    down = down.reshape(-1, width)
    up = up.reshape(-1, width)
    weight, grad, down, up = lax.optimization_barrier((weight, grad, down, up))
    last = segments - 1

    hidden = moved = x
    for k in range(last):
        hidden, x = forward_step(order, micro, tile, k, moved, x, gain, down, up, weight)
        moved = lax.ppermute(hidden, "segment", [(k, k + 1)])
    x = jnp.where(segment == last, moved, x)
    moved = grad
    for k in range(last, 0, -1):
        result, grad = backward_step(order, micro, k, moved, grad, x, gain, down, up, weight)
        moved = lax.ppermute(result, "segment", [(k, k - 1)])
        if k == last:
            hidden = lax.cond(
                segment == last,
                lambda: forward_step(order, micro, tile, last, x, x, gain, down, up, weight)[0],
                lambda: hidden,
            )
    both = sequence_step(members, micro, 0, moved, grad, x, gain, down, up)
    parts = lax.all_to_all(both, "dp", split_axis=0, concat_axis=0, tiled=True)
    grad_in, _ = backward_step(order, micro, 0, moved, grad, x, gain, down, up, weight)
    hidden = hidden.reshape(micro, rows, width)
    grad_in = grad_in.reshape(micro, rows, width)
    parts = parts.reshape(members, 2, micro, -1, width // members)
    mixed = jnp.einsum("mjs,jfmrd->fjsrd", mix_all, parts.astype(jnp.float32), precision=lax.Precision.HIGHEST)
    total = jnp.sum(mixed.astype(jnp.bfloat16).astype(jnp.float32), axis=1)
    return (hidden[None, :, None], grad_in[None, :, None], total[0][None], total[1][None])


def solution(mesh):
    in_specs = (
        P(None, "dp", None, None),
        P("segment", "dp", None),
        P("segment", None),
        P("segment", None, None, None),
        P("segment", None, None, None),
        P(),
        P(),
        P(),
        P(None, "dp", None, None),
    )
    out_specs = (
        P("segment", None, "dp", None, None),
        P("segment", None, "dp", None, None),
        P("segment", None, None, "dp"),
        P("segment", None, None, "dp"),
    )
    return jax.shard_map(shards, mesh=mesh, in_specs=in_specs, out_specs=out_specs, check_vma=False)
```
